1024 devices in a mesh: edp: 16 (over z), ep: 64 (over y, x, core).
Axes of the slice: x: 4, y: 8, z: 16, core: 2. Of those that a mesh axis runs over, the one named last changes fastest.
Arguments:
- out_grad: bfloat16 [131072, 3584], P(('edp', 'ep')), may hold values from -0.59765625 to 0.59765625
- routes: int32 [131072, 8], P(('edp', 'ep')), may hold values from 0 to 383, as said below
- gate_weights: float32 [131072, 8], P(('edp', 'ep')), may hold values from 0.02 to 0.5
- hidden: bfloat16 [8192, 16384], P('edp', 'ep'), may hold values from -6 to 6
Outputs:
- weight_grad: float32 [3584, 16384], P('edp', 'ep')
The draws below stay inside these ranges and needn't reach their ends.
Inputs may be any that keep to these rules, and one draw needn't show every extreme that they name: `routes`: each token names 8 different experts, at most one of them below 8. Among the tokens of one device no expert below 8 is named more than 8 times, and on every device one such expert, the same on all, is named exactly 8 times.
All inputs are finite; a program needn't handle non-finite values.
Results may differ from the reference program's by a relative error of at most 0.0029.
Values may be sent and summed in bfloat16 or wider, within the bound.
No kernel may reach another device: no remote copies, remote signals or barrier semaphores. Data moves between devices by JAX's collectives and lax.ppermute only.
A program may use at most 32 MiB of HBM per device.

```python
import math
import jax
import jax.numpy as jnp
from jax import lax

FEATURES = 3584
FF = 2048
ROUTED = 384
TOP = 8
CAP = 8
TOK_DEV = 128
EXPERTS = 8
SLOTS = 512
TOKENS = 131072
N_EDP = 16
N_EP = 64


def draw_routes(key, part):
    blocks = TOKENS // TOK_DEV
    subkeys = jax.random.split(jax.random.fold_in(key, 11), 5)
    counts = jax.random.randint(subkeys[0], (blocks, EXPERTS), CAP // 2, CAP + 1, dtype=jnp.int32)
    busiest = jax.random.randint(subkeys[1], (), 0, EXPERTS, dtype=jnp.int32)
    counts = jnp.where(jnp.arange(EXPERTS, dtype=jnp.int32)[None, :] == busiest, CAP, counts)
    block_ends = jnp.cumsum(counts, axis=1, dtype=jnp.int32)
    places = jnp.arange(TOK_DEV, dtype=jnp.int32)
    chosen = jnp.sum((places[None, :, None] >= block_ends[:, None, :]).astype(jnp.int32), axis=2, dtype=jnp.int32)

    def shuffle(subkey):
        return jax.random.permutation(subkey, TOK_DEV)
    orders = jax.vmap(shuffle)(jax.random.split(subkeys[2], blocks))
    chosen = jnp.take_along_axis(chosen, orders.astype(jnp.int32), axis=1)
    outside = ROUTED - EXPERTS
    offsets = jax.random.randint(subkeys[3], (blocks, TOK_DEV), 0, outside, dtype=jnp.int32)
    others = EXPERTS + (offsets[:, :, None] + jnp.arange(TOP, dtype=jnp.int32)[None, None, :]) % outside
    column = jax.random.randint(subkeys[4], (blocks, TOK_DEV), 0, TOP, dtype=jnp.int32)
    place_here = (chosen[:, :, None] < EXPERTS) & (jnp.arange(TOP, dtype=jnp.int32)[None, None, :] == column[:, :, None])
    result = jnp.where(place_here, chosen[:, :, None], others)
    return result.reshape(TOKENS, TOP).astype(jnp.int32)


def steps_of(key, dims, shards, least, high):
    def one(axis_at, blocks):
        steps = jax.random.uniform(jax.random.fold_in(jax.random.fold_in(key, 6), axis_at), (blocks,), jnp.float32, least / len(shards), high / len(shards))
        return jnp.repeat(jnp.exp(steps), dims[axis_at] // blocks).reshape((-1,) + (1,) * (len(dims) - axis_at - 1))

    loudness = one(*shards[0])
    for cut in shards[1:]:
        loudness = loudness * one(*cut)
    return loudness


def gaussian(stream_key, extent, deviation, bound, shards=(), kind=jnp.bfloat16):
    loudness = steps_of(stream_key, extent, shards, -0.22, 0.18) if shards else 1.0
    values = jax.random.normal(stream_key, extent, jnp.float32) * deviation * loudness
    return jnp.minimum(jnp.maximum(values, -bound), bound).astype(kind)


def setup_inputs(seed: int = 0) -> dict:
    key_list = jax.random.split(jax.random.key(seed), 5)
    return {
        "out_grad": gaussian(key_list[0], (TOKENS, FEATURES), 0.1, 0.59765625, ((0, 1024),)),
        "routes": draw_routes(jax.random.fold_in(key_list[4], 71), 0),
        "gate_weights": jnp.clip(jnp.exp(math.log(0.5) - 3.218876 * jax.random.uniform(key_list[2], (TOKENS, TOP), jnp.float32) ** steps_of(key_list[2], (TOKENS, TOP), ((0, 1024),), -0.2, 0.2)), 0.02, 0.5),
        "hidden": gaussian(key_list[3], (N_EDP * SLOTS, EXPERTS * FF), 1.0, 6.0, ((0, 16), (1, 64))),
    }


def dispatch(out_grad, routes, gate_weights):
    experts = EXPERTS
    labels = jnp.arange(experts, dtype=jnp.int32)
    onehot = jnp.sum((routes[:, :, None] == labels[None, None, :]).astype(jnp.int32), axis=1, dtype=jnp.int32)
    weight = jnp.sum(jnp.where(routes < experts, gate_weights, jnp.zeros_like(gate_weights)), axis=1)
    routed = (out_grad.astype(jnp.float32) * weight[:, None]).astype(jnp.bfloat16)
    slot_rank = jnp.cumsum(onehot, axis=0, dtype=jnp.int32) - onehot
    slot_index = jnp.sum(onehot * (labels[None, :] * CAP + slot_rank), axis=1, dtype=jnp.int32)
    is_live = jnp.sum(onehot, axis=1, dtype=jnp.int32)
    targets = jnp.arange(experts * CAP, dtype=jnp.int32)
    placer = ((is_live[None, :] == 1) & (slot_index[None, :] == targets[:, None])).astype(jnp.bfloat16)
    return jnp.dot(placer, routed, preferred_element_type=jnp.float32).astype(jnp.bfloat16)


def reference(out_grad, routes, gate_weights, hidden):
    grads = out_grad.reshape(N_EDP, N_EP, TOK_DEV, FEATURES)
    choices = routes.reshape(N_EDP, N_EP, TOK_DEV, TOP)
    weights = gate_weights.reshape(N_EDP, N_EP, TOK_DEV, TOP)
    saved = hidden.reshape(N_EDP, SLOTS, EXPERTS, FF)

    def replica_step(running, inputs):
        grad_part, choice_part, weight_part, saved_part = inputs
        outbound = jax.vmap(dispatch)(grad_part, choice_part, weight_part)
        slot_rows = outbound.reshape(N_EP, EXPERTS, CAP, FEATURES).transpose(1, 0, 2, 3).reshape(EXPERTS, SLOTS, FEATURES)
        partial_value = jnp.einsum("esd,sef->def", slot_rows.astype(jnp.float32), saved_part.astype(jnp.float32))
        partial_value = partial_value.reshape(FEATURES, EXPERTS * FF)
        return running + partial_value, None

    start = jnp.zeros((FEATURES, EXPERTS * FF), jnp.float32)
    result, _ = lax.scan(replica_step, start, (grads, choices, weights, saved))
    return result
```

```python
import jax
import jax.numpy as jnp
from jax import lax
from jax.experimental import pallas as pl
from jax.sharding import Mesh, PartitionSpec as P

CAP = 8
EXPERTS = 8
GROUP = 4


def place_kernel(grad_ref, routes_ref, gates_ref, out_ref):
    tokens, features = grad_ref.shape
    block = features // (GROUP * GROUP)
    routes = routes_ref[...]
    local = routes < EXPERTS
    weight = jnp.sum(jnp.where(local, gates_ref[...], 0.0), axis=1, keepdims=True)
    expert = jnp.sum(jnp.where(local, routes + 1, 0), axis=1, keepdims=True) - 1
    onehot = expert == lax.broadcasted_iota(jnp.int32, (tokens, 128), 1)
    earlier = lax.broadcasted_iota(jnp.int32, (tokens, tokens), 1) < lax.broadcasted_iota(
        jnp.int32, (tokens, tokens), 0
    )
    ranks = jnp.dot(
        earlier.astype(jnp.float32).astype(jnp.bfloat16),
        onehot.astype(jnp.float32).astype(jnp.bfloat16),
        preferred_element_type=jnp.float32,
    )
    rank = jnp.sum(jnp.where(onehot, ranks, 0.0), axis=1, keepdims=True).astype(jnp.int32)
    slot = jnp.where(expert >= 0, expert * CAP + rank, -1)
    placer = (slot == lax.broadcasted_iota(jnp.int32, (tokens, EXPERTS * CAP), 1)).astype(
        jnp.float32
    ).astype(jnp.bfloat16)
    routed = (grad_ref[...].astype(jnp.float32) * weight).astype(jnp.bfloat16)
    placed = lax.dot_general(
        placer, routed, (((0,), (0,)), ((), ())), preferred_element_type=jnp.float32
    )
    for low in range(GROUP):
        picked = jnp.concatenate(
            [
                placed[:, (high * GROUP + low) * block : (high * GROUP + low + 1) * block]
                for high in range(GROUP)
            ],
            axis=1,
        )
        out_ref[low] = picked.astype(jnp.bfloat16).reshape(EXPERTS, CAP, GROUP * block)


def place_rows(out_grad, routes, gate_weights):
    features = out_grad.shape[1]
    return pl.pallas_call(
        place_kernel,
        out_shape=jax.ShapeDtypeStruct(
            (GROUP, EXPERTS, CAP, features // GROUP), jnp.bfloat16
        ),
        cost_estimate=pl.CostEstimate(
            flops=2 * 64 * 128 * features, bytes_accessed=3 * 64 * 2 * features, transcendentals=0
        ),
    )(out_grad, routes, gate_weights)


def gradient(out_grad, routes, gate_weights, hidden):
    columns = hidden.shape[1]
    low, core = lax.axis_index("zl"), lax.axis_index("c")
    mine = hidden.reshape(EXPERTS, GROUP, 2, CAP, columns).transpose(2, 1, 0, 3, 4)
    mine = mine.reshape(2, GROUP, EXPERTS * CAP, columns)
    gathered = [mine]
    for step in (1, 2, 3):
        gathered.append(lax.ppermute(mine, "zl", [(i, i ^ step) for i in range(GROUP)]))
    stacked = jnp.stack(gathered)
    saved = jnp.stack(
        [lax.dynamic_index_in_dim(stacked, low ^ source, 0, False) for source in range(GROUP)],
        axis=2,
    )
    saved = saved.reshape(2, -1, columns)

    outbound = place_rows(out_grad, routes, gate_weights)
    features = outbound.shape[-1]
    outbound = outbound.reshape(GROUP * EXPERTS, CAP, features)
    arrived = lax.all_to_all(outbound, ("zl", "y"), split_axis=0, concat_axis=0, tiled=True)
    arrived = jnp.broadcast_to(
        arrived.reshape(1, -1, features), (GROUP, GROUP * EXPERTS * CAP, features)
    )
    rows = lax.all_to_all(arrived, "x", split_axis=0, concat_axis=0, tiled=True)
    rows = rows.reshape(-1, features)
    others = lax.ppermute(rows, "c", [(0, 1), (1, 0)])

    def product(part, which):
        return lax.dot_general(
            part,
            lax.dynamic_index_in_dim(saved, which, 0, False),
            (((0,), (0,)), ((), ())),
            preferred_element_type=jnp.float32,
        )

    partial = product(rows, core) + product(others, 1 - core)
    partial = partial.astype(jnp.bfloat16).reshape(GROUP, features // GROUP, columns)
    parts = lax.all_to_all(partial, "zh", split_axis=0, concat_axis=0, tiled=True)
    return jnp.sum(parts.astype(jnp.float32), axis=0)


def solution(mesh):
    axes = ("zh", "zl", "y", "x", "c")
    fine = Mesh(mesh.devices.reshape(GROUP, GROUP, EXPERTS, 4, 2), axes)
    tokens = P(axes, None)
    return jax.shard_map(
        gradient,
        mesh=fine,
        in_specs=(tokens, tokens, tokens, P(("zh", "zl"), ("y", "x", "c"))),
        out_specs=P(("zh", "zl"), ("y", "x", "c")),
        check_vma=False,
    )
```

```python
import jax
import jax.numpy as jnp
from jax import lax
from jax.experimental import pallas as pl
from jax.sharding import Mesh, PartitionSpec as P

CAP = 8
EXPERTS = 8
GROUP = 4


def place_kernel(grad_ref, routes_ref, gates_ref, out_ref):
    tokens, features = grad_ref.shape
    block = features // (GROUP * GROUP)
    routes = routes_ref[...]
    local = routes < EXPERTS
    weight = jnp.sum(jnp.where(local, gates_ref[...], 0.0), axis=0, keepdims=True)
    weight = jnp.transpose(jnp.broadcast_to(weight, (8, tokens)))[:, :1]
    expert = jnp.sum(jnp.where(local, routes + 1, 0), axis=0, keepdims=True) - 1
    onehot = expert == lax.broadcasted_iota(jnp.int32, (EXPERTS, tokens), 0)
    earlier = lax.broadcasted_iota(jnp.int32, (tokens, tokens), 0) < lax.broadcasted_iota(
        jnp.int32, (tokens, tokens), 1
    )
    ranks = jnp.dot(
        onehot.astype(jnp.float32).astype(jnp.bfloat16),
        earlier.astype(jnp.float32).astype(jnp.bfloat16),
        preferred_element_type=jnp.float32,
    )
    rank = jnp.sum(jnp.where(onehot, ranks, 0.0), axis=0, keepdims=True).astype(jnp.int32)
    slot = jnp.where(expert >= 0, expert * CAP + rank, -1)
    placer = (slot == lax.broadcasted_iota(jnp.int32, (EXPERTS * CAP, tokens), 0)).astype(
        jnp.float32
    ).astype(jnp.bfloat16)
    routed = (grad_ref[...].astype(jnp.float32) * weight).astype(jnp.bfloat16)
    placed = jnp.dot(placer, routed, preferred_element_type=jnp.float32)
    for low in range(GROUP):
        picked = jnp.concatenate(
            [
                placed[:, (high * GROUP + low) * block : (high * GROUP + low + 1) * block]
                for high in range(GROUP)
            ],
            axis=1,
        )
        out_ref[low] = picked.astype(jnp.bfloat16).reshape(EXPERTS, CAP, GROUP * block)


def place_rows(out_grad, routes, gate_weights):
    features = out_grad.shape[1]
    return pl.pallas_call(
        place_kernel,
        out_shape=jax.ShapeDtypeStruct(
            (GROUP, EXPERTS, CAP, features // GROUP), jnp.bfloat16
        ),
        cost_estimate=pl.CostEstimate(
            flops=2 * 64 * 128 * features, bytes_accessed=3 * 64 * 2 * features, transcendentals=0
        ),
    )(out_grad, routes.T, gate_weights.T)


def gradient(out_grad, routes, gate_weights, hidden):
    columns = hidden.shape[1]
    low, core = lax.axis_index("zl"), lax.axis_index("c")
    outbound = place_rows(out_grad, routes, gate_weights)
    features = outbound.shape[-1]
    outbound = outbound.reshape(GROUP * EXPERTS, CAP, features)
    arrived = lax.all_to_all(outbound, ("zl", "y"), split_axis=0, concat_axis=0, tiled=True)
    mine = hidden.reshape(EXPERTS, GROUP, 2, CAP, columns).transpose(2, 1, 0, 3, 4)
    mine = mine.reshape(2, GROUP, EXPERTS * CAP, columns)
    gathered = [mine]
    for step in (1, 2, 3):
        gathered.append(lax.ppermute(mine, "zl", [(i, i ^ step) for i in range(GROUP)]))
    stacked = jnp.stack(gathered)
    saved = jnp.stack(
        [lax.dynamic_index_in_dim(stacked, low ^ source, 0, False) for source in range(GROUP)],
        axis=2,
    )
    saved = saved.reshape(2, -1, columns)

    arrived = jnp.broadcast_to(
        arrived.reshape(1, -1, features), (GROUP, GROUP * EXPERTS * CAP, features)
    )
    rows = lax.all_to_all(arrived, "x", split_axis=0, concat_axis=0, tiled=True)
    rows = rows.reshape(-1, features)
    others = lax.ppermute(rows, "c", [(0, 1), (1, 0)])

    def product(part, which):
        return lax.dot_general(
            part,
            lax.dynamic_index_in_dim(saved, which, 0, False),
            (((0,), (0,)), ((), ())),
            preferred_element_type=jnp.float32,
        )

    partial = product(rows, core) + product(others, 1 - core)
    partial = partial.astype(jnp.bfloat16).reshape(GROUP, features // GROUP, columns)
    parts = lax.all_to_all(partial, "zh", split_axis=0, concat_axis=0, tiled=True)
    return jnp.sum(parts.astype(jnp.float32), axis=0)


def solution(mesh):
    axes = ("zh", "zl", "y", "x", "c")
    fine = Mesh(mesh.devices.reshape(GROUP, GROUP, EXPERTS, 4, 2), axes)
    tokens = P(axes, None)
    return jax.shard_map(
        gradient,
        mesh=fine,
        in_specs=(tokens, tokens, tokens, P(("zh", "zl"), ("y", "x", "c"))),
        out_specs=P(("zh", "zl"), ("y", "x", "c")),
        check_vma=False,
    )
```

```python
import jax
import jax.numpy as jnp
from jax import lax
from jax.experimental import pallas as pl
from jax.experimental.pallas import tpu as pltpu
from jax.sharding import Mesh, PartitionSpec as P

CAP = 8
EXPERTS = 8
GROUP = 4


def place_kernel(grad_in, routes_in, gates_in, out_ref, grad_ref, routes_ref, gates_ref, arrived):
    moves = [
        pltpu.make_async_copy(routes_in, routes_ref, arrived.at[0]),
        pltpu.make_async_copy(gates_in, gates_ref, arrived.at[1]),
        pltpu.make_async_copy(grad_in, grad_ref, arrived.at[2]),
    ]
    for move in moves:
        move.start()
    tokens, features = grad_ref.shape
    moves[0].wait()
    moves[1].wait()
    block = features // (GROUP * GROUP)
    routes = routes_ref[...]
    local = routes < EXPERTS
    weight = jnp.sum(jnp.where(local, gates_ref[...], 0.0), axis=0, keepdims=True)
    weight = jnp.transpose(jnp.broadcast_to(weight, (8, tokens)))[:, :1]
    expert = jnp.sum(jnp.where(local, routes + 1, 0), axis=0, keepdims=True) - 1
    onehot = expert == lax.broadcasted_iota(jnp.int32, (EXPERTS, tokens), 0)
    earlier = lax.broadcasted_iota(jnp.int32, (tokens, tokens), 0) < lax.broadcasted_iota(
        jnp.int32, (tokens, tokens), 1
    )
    ranks = jnp.dot(
        onehot.astype(jnp.float32).astype(jnp.bfloat16),
        earlier.astype(jnp.float32).astype(jnp.bfloat16),
        preferred_element_type=jnp.float32,
    )
    rank = jnp.sum(jnp.where(onehot, ranks, 0.0), axis=0, keepdims=True).astype(jnp.int32)
    slot = jnp.where(expert >= 0, expert * CAP + rank, -1)
    placer = (slot == lax.broadcasted_iota(jnp.int32, (EXPERTS * CAP, tokens), 0)).astype(
        jnp.float32
    ).astype(jnp.bfloat16)
    moves[2].wait()
    routed = (grad_ref[...].astype(jnp.float32) * weight).astype(jnp.bfloat16)
    placed = jnp.dot(placer, routed, preferred_element_type=jnp.float32)
    for low in range(GROUP):
        picked = jnp.concatenate(
            [
                placed[:, (high * GROUP + low) * block : (high * GROUP + low + 1) * block]
                for high in range(GROUP)
            ],
            axis=1,
        )
        out_ref[low] = picked.astype(jnp.bfloat16).reshape(EXPERTS, CAP, GROUP * block)


def place_rows(out_grad, routes, gate_weights):
    features = out_grad.shape[1]
    return pl.pallas_call(
        place_kernel,
        out_shape=jax.ShapeDtypeStruct(
            (GROUP, EXPERTS, CAP, features // GROUP), jnp.bfloat16
        ),
        in_specs=[pl.BlockSpec(memory_space=pltpu.HBM)] * 3,
        scratch_shapes=[
            pltpu.VMEM(out_grad.shape, out_grad.dtype),
            pltpu.VMEM(routes.shape[::-1], routes.dtype),
            pltpu.VMEM(gate_weights.shape[::-1], gate_weights.dtype),
            pltpu.SemaphoreType.DMA((3,)),
        ],
        cost_estimate=pl.CostEstimate(
            flops=2 * 64 * 128 * features, bytes_accessed=3 * 64 * 2 * features, transcendentals=0
        ),
    )(out_grad, routes.T, gate_weights.T)


def gradient(out_grad, routes, gate_weights, hidden):
    columns = hidden.shape[1]
    low, core = lax.axis_index("zl"), lax.axis_index("c")
    outbound = place_rows(out_grad, routes, gate_weights)
    features = outbound.shape[-1]
    outbound = outbound.reshape(GROUP * EXPERTS, CAP, features)
    arrived = lax.all_to_all(outbound, ("zl", "y"), split_axis=0, concat_axis=0, tiled=True)
    mine = hidden.reshape(EXPERTS, GROUP, 2, CAP, columns).transpose(2, 1, 0, 3, 4)
    mine = mine.reshape(2, GROUP, EXPERTS * CAP, columns)
    gathered = [mine]
    for step in (1, 2, 3):
        gathered.append(lax.ppermute(mine, "zl", [(i, i ^ step) for i in range(GROUP)]))
    stacked = jnp.stack(gathered)
    saved = jnp.stack(
        [lax.dynamic_index_in_dim(stacked, low ^ source, 0, False) for source in range(GROUP)],
        axis=2,
    )
    saved = saved.reshape(2, -1, columns)

    arrived = jnp.broadcast_to(
        arrived.reshape(1, -1, features), (GROUP, GROUP * EXPERTS * CAP, features)
    )
    rows = lax.all_to_all(arrived, "x", split_axis=0, concat_axis=0, tiled=True)
    rows = rows.reshape(-1, features)
    others = lax.ppermute(rows, "c", [(0, 1), (1, 0)])

    def product(part, which):
        return lax.dot_general(
            part,
            lax.dynamic_index_in_dim(saved, which, 0, False),
            (((0,), (0,)), ((), ())),
            preferred_element_type=jnp.float32,
        )

    partial = lax.optimization_barrier(product(rows, core))
    partial = partial + product(others, 1 - core)
    partial = partial.astype(jnp.bfloat16).reshape(GROUP, features // GROUP, columns)
    high = lax.axis_index("zh")

    def chunk(step):
        return lax.dynamic_index_in_dim(partial, high ^ step, 0, False)

    total = chunk(0).astype(jnp.float32)
    for step in (2, 3, 1):
        got = lax.ppermute(chunk(step), "zh", [(i, i ^ step) for i in range(GROUP)])
        total = total + got.astype(jnp.float32)
    return total


def solution(mesh):
    axes = ("zh", "zl", "y", "x", "c")
    fine = Mesh(mesh.devices.reshape(GROUP, GROUP, EXPERTS, 4, 2), axes)
    tokens = P(axes, None)
    return jax.shard_map(
        gradient,
        mesh=fine,
        in_specs=(tokens, tokens, tokens, P(("zh", "zl"), ("y", "x", "c"))),
        out_specs=P(("zh", "zl"), ("y", "x", "c")),
        check_vma=False,
    )
```

```python
import jax
import jax.numpy as jnp
from jax import lax
from jax.experimental import pallas as pl
from jax.experimental.pallas import tpu as pltpu
from jax.sharding import Mesh, PartitionSpec as P

CAP = 8
EXPERTS = 8
GROUP = 4


def place_kernel(grad_in, routes_in, gates_in, out_ref, grad_ref, routes_ref, gates_ref, arrived):
    moves = [
        pltpu.make_async_copy(routes_in, routes_ref, arrived.at[0]),
        pltpu.make_async_copy(gates_in, gates_ref, arrived.at[1]),
        pltpu.make_async_copy(grad_in, grad_ref, arrived.at[2]),
    ]
    for move in moves:
        move.start()
    tokens, features = grad_ref.shape
    moves[0].wait()
    moves[1].wait()
    block = features // (GROUP * GROUP)
    routes = routes_ref[...]
    local = routes < EXPERTS
    weight = jnp.sum(jnp.where(local, gates_ref[...], 0.0), axis=0, keepdims=True)
    weight = jnp.transpose(jnp.broadcast_to(weight, (8, tokens)))[:, :1]
    expert = jnp.sum(jnp.where(local, routes + 1, 0), axis=0, keepdims=True) - 1
    onehot = expert == lax.broadcasted_iota(jnp.int32, (EXPERTS, tokens), 0)
    earlier = lax.broadcasted_iota(jnp.int32, (tokens, tokens), 0) < lax.broadcasted_iota(
        jnp.int32, (tokens, tokens), 1
    )
    ranks = jnp.dot(
        onehot.astype(jnp.float32).astype(jnp.bfloat16),
        earlier.astype(jnp.float32).astype(jnp.bfloat16),
        preferred_element_type=jnp.float32,
    )
    rank = jnp.sum(jnp.where(onehot, ranks, 0.0), axis=0, keepdims=True).astype(jnp.int32)
    slot = jnp.where(expert >= 0, expert * CAP + rank, -1)
    placer = (slot == lax.broadcasted_iota(jnp.int32, (EXPERTS * CAP, tokens), 0)).astype(
        jnp.float32
    ).astype(jnp.bfloat16)
    moves[2].wait()
    routed = (grad_ref[...].astype(jnp.float32) * weight).astype(jnp.bfloat16)
    placed = jnp.dot(placer, routed, preferred_element_type=jnp.float32)
    for low in range(GROUP):
        picked = jnp.concatenate(
            [
                placed[:, (high * GROUP + low) * block : (high * GROUP + low + 1) * block]
                for high in range(GROUP)
            ],
            axis=1,
        )
        out_ref[low] = picked.astype(jnp.bfloat16).reshape(EXPERTS, CAP, GROUP * block)


def place_rows(out_grad, routes, gate_weights):
    features = out_grad.shape[1]
    return pl.pallas_call(
        place_kernel,
        out_shape=jax.ShapeDtypeStruct(
            (GROUP, EXPERTS, CAP, features // GROUP), jnp.bfloat16
        ),
        in_specs=[pl.BlockSpec(memory_space=pltpu.HBM)] * 3,
        scratch_shapes=[
            pltpu.VMEM(out_grad.shape, out_grad.dtype),
            pltpu.VMEM(routes.shape[::-1], routes.dtype),
            pltpu.VMEM(gate_weights.shape[::-1], gate_weights.dtype),
            pltpu.SemaphoreType.DMA((3,)),
        ],
        cost_estimate=pl.CostEstimate(
            flops=2 * 64 * 128 * features, bytes_accessed=3 * 64 * 2 * features, transcendentals=0
        ),
    )(out_grad, routes.T, gate_weights.T)


def gradient(out_grad, routes, gate_weights, hidden):
    columns = hidden.shape[1]
    low, core = lax.axis_index("zl"), lax.axis_index("c")
    outbound = place_rows(out_grad, routes, gate_weights)
    features = outbound.shape[-1]
    outbound = outbound.reshape(GROUP * EXPERTS, CAP, features)
    arrived = lax.all_to_all(outbound, ("zl", "y"), split_axis=0, concat_axis=0, tiled=True)
    mine = hidden.reshape(EXPERTS, GROUP, 2, CAP, columns).transpose(2, 1, 0, 3, 4)
    mine = jnp.concatenate([mine, mine], axis=0)
    mine = lax.dynamic_slice_in_dim(mine, core, 2, axis=0)
    mine = jnp.concatenate([mine, mine], axis=1)
    mine = lax.dynamic_slice_in_dim(mine, lax.axis_index("x"), GROUP, axis=1)
    mine = mine.reshape(2, GROUP, EXPERTS * CAP, columns)
    gathered = [mine]
    for step in (1, 2, 3):
        gathered.append(lax.ppermute(mine, "zl", [(i, i ^ step) for i in range(GROUP)]))
    stacked = jnp.stack(gathered)
    saved = jnp.stack(
        [lax.dynamic_index_in_dim(stacked, low ^ source, 0, False) for source in range(GROUP)],
        axis=2,
    )
    saved = saved.reshape(2, GROUP, -1, columns)

    def from_x(part, step):
        return lax.ppermute(part, "x", [((i + step) % GROUP, i) for i in range(GROUP)])

    arrived = arrived.reshape(-1, features)
    half = arrived.shape[0] // 2
    after, before = from_x(arrived, 1), from_x(arrived, 3)
    through = after[:half], before[half:]
    opposite = [from_x(through[0], 1), from_x(through[1], 3)]
    near = jnp.concatenate([arrived, after, before])
    far = jnp.concatenate(opposite)
    swapped = []
    for part in (near, far):
        swapped.append(lax.ppermute(part, "c", [(0, 1), (1, 0)]))

    def product(part, which):
        return lax.dot_general(
            part, which, (((0,), (0,)), ((), ())), preferred_element_type=jnp.float32
        )

    close = jnp.concatenate([saved[:, :2], saved[:, 3:]], axis=1).reshape(2, -1, columns)
    partial = product(near, close[0]) + product(far, saved[0, 2])
    partial = lax.optimization_barrier(partial)
    partial = lax.optimization_barrier(partial + product(swapped[0], close[1]))
    partial = partial + product(swapped[1], saved[1, 2])
    partial = partial.astype(jnp.bfloat16).reshape(GROUP, features // GROUP, columns)
    high = lax.axis_index("zh")

    def chunk(step):
        return lax.dynamic_index_in_dim(partial, high ^ step, 0, False)

    total = chunk(0).astype(jnp.float32)
    for step in (3, 2, 1):
        got = lax.ppermute(chunk(step), "zh", [(i, i ^ step) for i in range(GROUP)])
        total = total + got.astype(jnp.float32)
    return total


def solution(mesh):
    axes = ("zh", "zl", "y", "x", "c")
    fine = Mesh(mesh.devices.reshape(GROUP, GROUP, EXPERTS, 4, 2), axes)
    tokens = P(axes, None)
    return jax.shard_map(
        gradient,
        mesh=fine,
        in_specs=(tokens, tokens, tokens, P(("zh", "zl"), ("y", "x", "c"))),
        out_specs=P(("zh", "zl"), ("y", "x", "c")),
        check_vma=False,
    )
```
